32 devices in a mesh: fsdp: 16 (over z, y, core), tp: 2 (over x).
Axes of the slice: x: 2, y: 2, z: 4, core: 2. Of those that a mesh axis runs over, the one named last changes fastest.
Arguments:
- inputs: bfloat16 [2, 16384, 768], P(None, ('fsdp', 'tp')), may hold values from -60 to 60
- image_ids: int32 [2, 16384], P(None, ('fsdp', 'tp')), may hold values from 0 to 127, never falling along the last dimension, each value on 1 to 256 neighbouring positions
- cotangent: bfloat16 [2, 16384, 768], P(None, ('fsdp', 'tp')), may hold values from -36 to 36
- norm1_gain: float32 [768], replicated, may hold values from 0.25 to 1.75
- norm1_bias: float32 [768], replicated, may hold values from -3 to 3
- qkv_weight: bfloat16 [768, 3, 768], P('fsdp', None, 'tp'), may hold values from -0.21875 to 0.21875
- qkv_bias: float32 [3, 768], P(None, 'tp'), may hold values from -3 to 3
- query_gain: float32 [64], replicated, may hold values from 0.25 to 1.75
- query_bias: float32 [64], replicated, may hold values from -3 to 3
- key_gain: float32 [64], replicated, may hold values from 0.25 to 1.75
- out_weight: bfloat16 [768, 768], P('tp', 'fsdp'), may hold values from -0.875 to 0.875
- out_bias: float32 [768], replicated, may hold values from -3 to 3
- norm2_gain: float32 [768], replicated, may hold values from 0.25 to 1.75
- norm2_bias: float32 [768], replicated, may hold values from -3 to 3
- up_weight: bfloat16 [768, 3072], P('fsdp', 'tp'), may hold values from -0.21875 to 0.21875
- up_bias: float32 [3072], P('tp'), may hold values from -3 to 3
- down_weight: bfloat16 [3072, 768], P('tp', 'fsdp'), may hold values from -0.109375 to 0.109375
- down_bias: float32 [768], replicated, may hold values from -3 to 3
Outputs:
- output: bfloat16 [2, 16384, 768], P(None, ('fsdp', 'tp'))
- input_grad: float32 [2, 16384, 768], P(None, ('fsdp', 'tp'))
- norm1_gain_grad: float32 [768], replicated
- norm1_bias_grad: float32 [768], replicated
- qkv_weight_grad: float32 [768, 3, 768], P('fsdp', None, 'tp')
- qkv_bias_grad: float32 [3, 768], P(None, 'tp')
- query_gain_grad: float32 [64], replicated
- query_bias_grad: float32 [64], replicated
- key_gain_grad: float32 [64], replicated
- out_weight_grad: float32 [768, 768], P('tp', 'fsdp')
- out_bias_grad: float32 [768], replicated
- norm2_gain_grad: float32 [768], replicated
- norm2_bias_grad: float32 [768], replicated
- up_weight_grad: float32 [768, 3072], P('fsdp', 'tp')
- up_bias_grad: float32 [3072], P('tp')
- down_weight_grad: float32 [3072, 768], P('tp', 'fsdp')
- down_bias_grad: float32 [768], replicated
The draws below stay inside these ranges and needn't reach their ends.
Inputs may be any that keep to these rules, and one draw needn't show every extreme that they name: `image_ids`: along each micro-batch's row of 16384 tokens the image ids never fall; every image has 1 to 256 tokens, and one has exactly 256.
All inputs are finite; a program needn't handle non-finite values.
Results may differ from the reference program's by a relative error of at most 0.01.
Values may be sent and summed in bfloat16 or wider, within the bound.
A program may use at most 192 MiB of HBM per device.

```python
import math
import jax
import jax.numpy as jnp
import numpy as np
from jax import lax

D = 768
HEADS = 12
HD = 64
FF = 3072
LEN = 1024
MB = 2
IMG_MOST = 256
TOK = 16384
IMAGES = 128


def draw_inputs(key, part):
    first, second, third = jax.random.split(key, 3)
    row_level = jax.random.uniform(second, (MB, TOK, 1), jnp.float32)
    column_level = jax.random.uniform(third, (1, 1, D), jnp.float32)
    scales = jnp.exp((row_level - 0.5) * math.log(10.0)) * jnp.exp((column_level - 0.5) * math.log(10.0))
    base = jax.random.normal(first, (MB, TOK, D), jnp.float32)
    return (jnp.clip(base, -6.0, 6.0) * scales).astype(jnp.bfloat16)


def draw_cotangent(key, part):
    first = jax.random.fold_in(key, 0)
    position = lax.broadcasted_iota(jnp.float32, (MB, TOK, 1), 1) / max(TOK - 1, 1)
    rising = 1.0 + 2.0 * position
    base = jnp.clip(jax.random.normal(first, (MB, TOK, D), jnp.float32), -6.0, 6.0)
    return (base * rising).astype(jnp.bfloat16)


def shard_levels(stream_key, dims, cuts, low, high):
    def one(axis_at, parts):
        draws = jax.random.uniform(jax.random.fold_in(jax.random.fold_in(stream_key, 6), axis_at), (parts,), jnp.float32, low / len(cuts), high / len(cuts))
        return jnp.repeat(jnp.exp(draws), dims[axis_at] // parts).reshape((-1,) + (1,) * (len(dims) - axis_at - 1))

    level = one(*cuts[0])
    for cut in cuts[1:]:
        level = level * one(*cut)
    return level


def profile(count, total, most, slope):
    loads = [(1 << 20) // math.isqrt(standing ** slope) + 1 for standing in range(2, count + 1)]
    surplus, holding = total - most - (count - 1), [1] * (count - 1)
    while surplus > 0:
        free = [i for i in range(count - 1) if holding[i] < most]
        whole, remaining = sum([loads[i] for i in free]), surplus
        for i in free:
            addition = min(most - holding[i], max(1, remaining * loads[i] // whole), surplus)
            holding[i] = holding[i] + addition
            surplus = surplus - addition
    return np.array([most] + holding)


def ragged_sizes(key, amount, total, limit, slope):
    if amount == 2:
        one = jax.random.randint(key, (), max(1, total - limit), min(limit, total - 1) + 1)
        return jnp.stack([one, total - one])
    sizes = jnp.asarray(profile(amount, total, limit, slope), jnp.int32)
    twos = (amount - 1) // 2
    giver, taker = sizes[1:1 + 2 * twos:2], sizes[2:2 + 2 * twos:2]
    room = jnp.minimum(giver - 1, limit - taker)
    passed = jax.random.randint(jax.random.fold_in(key, 1), (twos,), 0, 1 << 20) % (room + 1)
    sizes = sizes.at[1:1 + 2 * twos:2].set(giver - passed).at[2:2 + 2 * twos:2].set(taker + passed)
    return sizes[jax.random.permutation(jax.random.fold_in(key, 2), amount)]


def normal_values(rng, shape, deviation, reach, cuts=(), held_as=jnp.bfloat16):
    factor_of = shard_levels(rng, shape, cuts, -0.22, 0.18) if cuts else 1.0
    drawn = jax.random.normal(rng, shape, jnp.float32) * deviation * factor_of
    return jnp.minimum(jnp.maximum(drawn, -reach), reach).astype(held_as)


def setup_inputs(seed: int = 0) -> dict:
    streams_of = jax.random.split(jax.random.key(seed), 19)
    inputs = draw_inputs(jax.random.fold_in(streams_of[18], 71), 0)
    image_ids = jax.vmap(lambda own: jnp.searchsorted(jnp.cumsum(ragged_sizes(own, IMAGES, TOK, IMG_MOST, 2)), jnp.arange(TOK), side="right"))(jax.random.split(streams_of[1], MB)).reshape((MB, TOK)).astype(jnp.int32)
    cotangent = draw_cotangent(jax.random.fold_in(streams_of[18], 71), 0)
    norm1_gain = jnp.clip(1.0 + 0.15 * jax.random.normal(streams_of[3], (D,), jnp.float32), 0.25, 1.75)
    norm1_bias = normal_values(streams_of[4], (D,), 0.3, 3.0, (), jnp.float32)
    qkv_weight = normal_values(streams_of[5], (D, 3, D), D ** -0.5, 0.21875, ((0, 16), (2, 2)))
    qkv_bias = normal_values(streams_of[6], (3, D), 0.5, 3.0, ((1, 2),), jnp.float32)
    query_gain = jnp.clip(1.0 + 0.15 * jax.random.normal(streams_of[7], (HD,), jnp.float32), 0.25, 1.75)
    query_bias = normal_values(streams_of[8], (HD,), 0.3, 3.0, (), jnp.float32)
    key_gain = jnp.clip(1.0 + 0.15 * jax.random.normal(streams_of[9], (HD,), jnp.float32), 0.25, 1.75)
    out_weight = normal_values(streams_of[10], (D, D), (D // 16) ** -0.5, 0.875, ((0, 2), (1, 16)))
    out_bias = normal_values(streams_of[11], (D,), 0.5, 3.0, (), jnp.float32)
    norm2_gain = jnp.clip(1.0 + 0.15 * jax.random.normal(streams_of[12], (D,), jnp.float32), 0.25, 1.75)
    norm2_bias = normal_values(streams_of[13], (D,), 0.3, 3.0, (), jnp.float32)
    up_weight = normal_values(streams_of[14], (D, FF), D ** -0.5, 0.21875, ((0, 16), (1, 2)))
    up_bias = normal_values(streams_of[15], (FF,), 0.5, 3.0, ((0, 2),), jnp.float32)
    down_weight = normal_values(streams_of[16], (FF, D), FF ** -0.5, 0.109375, ((0, 2), (1, 16)))
    down_bias = normal_values(streams_of[17], (D,), 0.5, 3.0, (), jnp.float32)
    return {"inputs": inputs, "image_ids": image_ids, "cotangent": cotangent, "norm1_gain": norm1_gain, "norm1_bias": norm1_bias, "qkv_weight": qkv_weight, "qkv_bias": qkv_bias, "query_gain": query_gain, "query_bias": query_bias, "key_gain": key_gain, "out_weight": out_weight, "out_bias": out_bias, "norm2_gain": norm2_gain, "norm2_bias": norm2_bias, "up_weight": up_weight, "up_bias": up_bias, "down_weight": down_weight, "down_bias": down_bias}


@jax.custom_vjp
def low(v):
    return lax.optimization_barrier(v.astype(jnp.bfloat16)).astype(jnp.float32)

@jax.custom_vjp
def low_back(v):
    return v

def low_keep(v):
    return (low(v), None)

def low_pass(kept, grad):
    return (grad,)

def back_keep(v):
    return (v, None)

def back_low(kept, grad):
    return (low(grad),)
low.defvjp(low_keep, low_pass)
low_back.defvjp(back_keep, back_low)
EPSILON = 1e-06
HIGHEST = lax.Precision.HIGHEST

def layer_norm(values, gain, shift):
    average = lax.optimization_barrier(jnp.mean(values, axis=-1, keepdims=True))
    centred = values - average
    spread = lax.optimization_barrier(jnp.mean(centred * centred, axis=-1, keepdims=True))
    return centred * lax.rsqrt(spread + EPSILON) * gain + shift

def attend_group(pieces):
    queries, keys, values, group_ids = pieces
    scale = HD ** (-0.5)
    scores = jnp.einsum('sqhd,skhd->shqk', queries, keys, precision=HIGHEST) * scale
    scores = low_back(scores)
    same = group_ids[:, None, :, None] == group_ids[:, None, None, :]
    masked = jnp.where(same, scores, -1e+30)
    weights = jnp.exp(masked - jax.nn.logsumexp(masked, axis=-1, keepdims=True))
    weights = low(weights)
    return jnp.einsum('shqk,skhd->sqhd', weights, values, precision=HIGHEST)

def block_forward(tokens_in, token_ids, params):
    norm1_gain, norm1_bias, qkv_weight, qkv_bias, query_gain, query_bias, key_gain, out_weight, out_bias, norm2_gain, norm2_bias, up_weight, up_bias, down_weight, down_bias = params
    count = tokens_in.shape[0]
    normed1 = low(layer_norm(tokens_in, norm1_gain, norm1_bias))
    project = jnp.dot(normed1, qkv_weight.reshape(D, 3 * D), precision=HIGHEST) + qkv_bias.reshape(3 * D)
    project = low_back(project).reshape(count, 3, HEADS, HD)
    queries = low(layer_norm(project[:, 0], query_gain, query_bias))
    keys = low(layer_norm(project[:, 1], key_gain, 0.0))
    values = low(project[:, 2])
    seq_total = count // LEN
    together = math.gcd(seq_total, max(1, 4096 // LEN))
    groups = seq_total // together
    shaped = (groups, together, LEN, HEADS, HD)
    mixed = lax.map(jax.checkpoint(attend_group), (queries.reshape(shaped), keys.reshape(shaped), values.reshape(shaped), token_ids.reshape(groups, together, LEN)))
    mixed = low(low_back(mixed.reshape(count, D)))
    attended = low_back(jnp.dot(mixed, out_weight, precision=HIGHEST))
    resid = tokens_in + attended + out_bias
    normed2 = low(layer_norm(resid, norm2_gain, norm2_bias))
    preact = low_back(jnp.dot(normed2, up_weight, precision=HIGHEST) + up_bias)
    hidden = low(jax.nn.gelu(preact, approximate=False))
    branch = low_back(jnp.dot(hidden, down_weight, precision=HIGHEST))
    return resid + branch + down_bias

def reference(inputs, image_ids, cotangent, norm1_gain, norm1_bias, qkv_weight, qkv_bias, query_gain, query_bias, key_gain, out_weight, out_bias, norm2_gain, norm2_bias, up_weight, up_bias, down_weight, down_bias):
    params = tuple((p.astype(jnp.float32) for p in (norm1_gain, norm1_bias, qkv_weight, qkv_bias, query_gain, query_bias, key_gain, out_weight, out_bias, norm2_gain, norm2_bias, up_weight, up_bias, down_weight, down_bias)))
    outputs = []
    in_grads = []
    totals = None
    for batch in range(MB):
        tokens_in = inputs[batch].astype(jnp.float32)
        token_ids = image_ids[batch].astype(jnp.int32)
        result, pullback = jax.vjp(lambda xin, prm: block_forward(xin, token_ids, prm), tokens_in, params)
        grad_in, grad_params = pullback(cotangent[batch].astype(jnp.float32))
        outputs.append(result.astype(jnp.bfloat16))
        in_grads.append(grad_in)
        if totals is None:
            totals = grad_params
        else:
            totals = tuple((a + b for a, b in zip(totals, grad_params)))
    g_n1g, g_n1b, g_qkvw, g_qkvb, g_qg, g_qb, g_kg, g_ow, g_ob, g_n2g, g_n2b, g_uw, g_ub, g_dw, g_db = totals
    return (jnp.stack(outputs), jnp.stack(in_grads), g_n1g, g_n1b, g_qkvw, g_qkvb, g_qg, g_qb, g_kg, g_ow, g_ob, g_n2g, g_n2b, g_uw, g_ub, g_dw, g_db)
```

```python
from functools import partial

import jax
import jax.numpy as jnp
from jax import lax
from jax.experimental import pallas as pl
from jax.experimental.pallas import tpu as pltpu
from jax.sharding import PartitionSpec as P

LEN = 1024
IMG_MOST = 256
BLOCK = 256
REACH = -(-(IMG_MOST - 1) // BLOCK)
EPSILON = 1e-06
BF = jnp.bfloat16
F32 = jnp.float32


def norm_parts(values):
    average = jnp.mean(values, axis=-1, keepdims=True)
    centred = values - average
    spread = jnp.mean(centred * centred, axis=-1, keepdims=True)
    scaled = lax.rsqrt(spread + EPSILON)
    return (centred * scaled, scaled)


def norm_back(grad_out, unit, scaled, gain):
    grad_unit = grad_out * gain
    first = jnp.mean(grad_unit, axis=-1, keepdims=True)
    second = jnp.mean(grad_unit * unit, axis=-1, keepdims=True)
    return scaled * (grad_unit - first - unit * second)


def mm(a, b):
    return jnp.dot(a, b, preferred_element_type=F32)


def mm_nt(a, b):
    return lax.dot_general(a, b, (((1,), (1,)), ((), ())), preferred_element_type=F32)


def mm_tn(a, b):
    return lax.dot_general(a, b, (((0,), (0,)), ((), ())), preferred_element_type=F32)


def key_range(block, count):
    return max(0, block - REACH), min(count, block + REACH + 1)


def attend_kernel(
    x_ref, w_ref, b_ref, qg_ref, qb_ref, kg_ref, idc_ref, idr_ref, p_ref, mixed_ref, *, depth
):
    length = x_ref.shape[0]
    lanes = mixed_ref.shape[1]
    count = length // BLOCK
    scale = depth ** (-0.5)
    project = mm(x_ref[...], w_ref[0]) + b_ref[0]
    p_ref[0] = project
    heads = []
    for head in range(lanes // depth):
        part = [
            project[:, i * lanes + head * depth : i * lanes + (head + 1) * depth] for i in range(3)
        ]
        query = (norm_parts(part[0])[0] * qg_ref[...] + qb_ref[...]).astype(BF)
        query = query * jnp.asarray(scale, BF)
        key = (norm_parts(part[1])[0] * kg_ref[...]).astype(BF)
        value = part[2].astype(BF)
        value = jnp.concatenate([value, jnp.ones_like(value)], axis=1)
        rows = []
        for block in range(count):
            low, high = key_range(block, count)
            q = slice(block * BLOCK, (block + 1) * BLOCK)
            k = slice(low * BLOCK, high * BLOCK)
            scores = mm_nt(query[q], key[k])
            same = idc_ref[q, :] == idr_ref[:, k]
            weights = jnp.where(same, jnp.exp(scores), 0.0).astype(BF)
            both = mm(weights, value[k])
            rows.append(both[:, :depth] / both[:, depth : depth + 1])
        heads.append(jnp.concatenate(rows, axis=0))
    mixed_ref[...] = jnp.concatenate(heads, axis=1).astype(BF)


def attend_back_kernel(
    g_ref, w_ref, p_ref, qg_ref, qb_ref, kg_ref, idc_ref, idr_ref, gp_ref, sums_ref, *, depth
):
    length = g_ref.shape[0]
    lanes = w_ref.shape[2]
    count = length // BLOCK
    scale = depth ** (-0.5)
    grad_mixed = mm(g_ref[...], w_ref[0]).astype(BF)
    project = p_ref[0]
    sums = [jnp.zeros((1, depth), F32) for _ in range(3)]
    columns = [[], [], []]
    for head in range(lanes // depth):
        part = [
            project[:, i * lanes + head * depth : i * lanes + (head + 1) * depth] for i in range(3)
        ]
        query_unit, query_scaled = norm_parts(part[0])
        key_unit, key_scaled = norm_parts(part[1])
        query = (query_unit * qg_ref[...] + qb_ref[...]).astype(BF)
        query = query * jnp.asarray(scale, BF)
        key = (key_unit * kg_ref[...]).astype(BF)
        value = part[2].astype(BF)
        grad = grad_mixed[:, head * depth : (head + 1) * depth]
        grad_key = [None] * count
        grad_value = [None] * count
        grad_query = []
        for block in range(count):
            low, high = key_range(block, count)
            q = slice(block * BLOCK, (block + 1) * BLOCK)
            k = slice(low * BLOCK, high * BLOCK)
            scores = mm_nt(key[k], query[q])
            same = idc_ref[k, :] == idr_ref[:, q]
            raised = jnp.where(same, jnp.exp(scores), 0.0)
            weights = raised * (1.0 / jnp.sum(raised, axis=0, keepdims=True))
            grad_weights = mm_nt(value[k], grad[q])
            inner = jnp.sum(grad_weights * weights, axis=0, keepdims=True)
            grad_scores = (weights * (grad_weights - inner)).astype(BF)
            grad_query.append(mm_tn(grad_scores, key[k]) * scale)
            to_key = mm(grad_scores, query[q])
            to_value = mm(weights.astype(BF), grad[q])
            for i in range(low, high):
                piece = slice((i - low) * BLOCK, (i - low + 1) * BLOCK)
                grad_key[i] = to_key[piece] if grad_key[i] is None else grad_key[i] + to_key[piece]
                grad_value[i] = (
                    to_value[piece] if grad_value[i] is None else grad_value[i] + to_value[piece]
                )
        grad_query = jnp.concatenate(grad_query, axis=0)
        grad_key = jnp.concatenate(grad_key, axis=0)
        grad_value = jnp.concatenate(grad_value, axis=0)
        sums[0] += jnp.sum(grad_query * query_unit, axis=0, keepdims=True)
        sums[1] += jnp.sum(grad_query, axis=0, keepdims=True)
        sums[2] += jnp.sum(grad_key * key_unit, axis=0, keepdims=True)
        columns[0].append(norm_back(grad_query, query_unit, query_scaled, qg_ref[...]))
        columns[1].append(norm_back(grad_key, key_unit, key_scaled, kg_ref[...]))
        columns[2].append(grad_value)
    for i in range(3):
        gp_ref[0, :, i * lanes : (i + 1) * lanes] = jnp.concatenate(columns[i], axis=1).astype(BF)

    @pl.when(pl.program_id(0) == 0)
    def _():
        sums_ref[...] = jnp.zeros_like(sums_ref)

    for i in range(3):
        sums_ref[i : i + 1, :] += sums[i]


def attend(normed, weight, bias, query_gain, query_bias, key_gain, ids, local_width):
    length, width = normed.shape
    tp = weight.shape[0]
    depth = query_gain.shape[0]
    lanes = 2 * depth
    per = local_width // lanes
    whole = lambda *shape: pl.BlockSpec(shape, lambda i: (0,) * len(shape))
    return pl.pallas_call(
        partial(attend_kernel, depth=depth),
        grid=(tp * per,),
        in_specs=[
            whole(length, width),
            pl.BlockSpec((1, width, 3 * lanes), lambda i: (i // per, 0, i % per)),
            pl.BlockSpec((1, 1, 3 * lanes), lambda i: (i // per, 0, i % per)),
            whole(1, depth),
            whole(1, depth),
            whole(1, depth),
            whole(length, 1),
            whole(1, length),
        ],
        out_specs=[
            pl.BlockSpec((1, length, 3 * lanes), lambda i: (i // per, 0, i % per)),
            pl.BlockSpec((length, lanes), lambda i: (0, i)),
        ],
        out_shape=[
            jax.ShapeDtypeStruct((tp, length, 3 * local_width), F32),
            jax.ShapeDtypeStruct((length, tp * local_width), BF),
        ],
        compiler_params=pltpu.CompilerParams(vmem_limit_bytes=56 * 2**20),
        cost_estimate=pl.CostEstimate(
            flops=2 * length * width * 3 * local_width * tp,
            bytes_accessed=length * local_width * tp * 16,
            transcendentals=length * 3 * BLOCK * tp * local_width // depth,
        ),
        name="attend",
    )(
        normed,
        weight,
        bias,
        query_gain[None],
        query_bias[None],
        key_gain[None],
        ids[:, None],
        ids[None],
    )


def attend_back(
    grad_rows, weight, out_column, project, query_gain, query_bias, key_gain, ids, local_width
):
    length, width = grad_rows.shape
    tp = weight.shape[0]
    depth = query_gain.shape[0]
    lanes = 2 * depth
    per = local_width // lanes
    first = out_column // lanes
    whole = lambda *shape: pl.BlockSpec(shape, lambda i: (0,) * len(shape))
    return pl.pallas_call(
        partial(attend_back_kernel, depth=depth),
        grid=(tp * per,),
        in_specs=[
            whole(length, width),
            pl.BlockSpec((1, width, lanes), lambda i: (i // per, 0, first + i % per)),
            pl.BlockSpec((1, length, 3 * lanes), lambda i: (i // per, 0, i % per)),
            whole(1, depth),
            whole(1, depth),
            whole(1, depth),
            whole(length, 1),
            whole(1, length),
        ],
        out_specs=[
            pl.BlockSpec((1, length, 3 * lanes), lambda i: (i // per, 0, i % per)),
            whole(3, depth),
        ],
        out_shape=[
            jax.ShapeDtypeStruct((tp, length, 3 * local_width), BF),
            jax.ShapeDtypeStruct((3, depth), F32),
        ],
        compiler_params=pltpu.CompilerParams(vmem_limit_bytes=56 * 2**20),
        cost_estimate=pl.CostEstimate(
            flops=8 * length * width * local_width * tp,
            bytes_accessed=length * local_width * tp * 18,
            transcendentals=length * 3 * BLOCK * tp * local_width // depth,
        ),
        name="attend_back",
    )(
        grad_rows,
        weight,
        project,
        query_gain[None],
        query_bias[None],
        key_gain[None],
        ids[:, None],
        ids[None],
    )


def on_device(
    inputs,
    image_ids,
    cotangent,
    norm1_gain,
    norm1_bias,
    qkv_weight,
    qkv_bias,
    query_gain,
    query_bias,
    key_gain,
    out_weight,
    out_bias,
    norm2_gain,
    norm2_bias,
    up_weight,
    up_bias,
    down_weight,
    down_bias,
):
    batches, rows_here, width = inputs.shape
    tp = lax.axis_size("tp")
    me = lax.axis_index("tp")
    assert batches == 2 and tp == 2 and rows_here * tp == LEN
    everyone = ("tp", "fsdp")
    shard = qkv_weight.shape[0]
    local_width = qkv_weight.shape[2]
    local_hidden = up_weight.shape[1]
    lanes = 2 * query_gain.shape[0]
    per = local_width // lanes
    swap = [(0, 1), (1, 0)]

    def pick(array, index):
        return lax.dynamic_index_in_dim(array, index, 0, keepdims=False)

    def in_order(own, other):
        return jnp.where(
            me == 0, jnp.concatenate([own, other], 0), jnp.concatenate([other, own], 0)
        )

    def to_sequence(array):
        return in_order(pick(array, me), lax.ppermute(pick(array, 1 - me), "tp", swap))

    def from_sequence(array, dtype):
        halves = array.reshape(2, rows_here, width)
        other = lax.ppermute(pick(halves, 1 - me).astype(dtype), "tp", swap).astype(array.dtype)
        own = pick(halves, me)
        return jnp.where(me == 0, jnp.stack([own, other]), jnp.stack([other, own]))

    packed = jnp.concatenate(
        [
            qkv_weight.reshape(shard, 3, per, lanes).transpose(0, 2, 1, 3).reshape(shard, -1),
            out_weight.T,
            up_weight,
            down_weight.T,
        ],
        axis=1,
    )
    gathered = lax.all_gather(packed, everyone, axis=0, tiled=True).reshape(tp, width, -1)
    edge_out = 3 * local_width
    edge_up = edge_out + local_width
    edge_down = edge_up + local_hidden
    out_t = [gathered[i, :, edge_out:edge_up] for i in range(tp)]
    up = [gathered[i, :, edge_up:edge_down] for i in range(tp)]
    down_t = [gathered[i, :, edge_down:] for i in range(tp)]
    qkv = [gathered[i, :, :edge_out] for i in range(tp)]

    biases = jnp.concatenate(
        [qkv_bias.reshape(3, per, lanes).transpose(1, 0, 2).reshape(-1), up_bias]
    )
    biases = in_order(biases[None], lax.ppermute(biases, "tp", swap)[None])
    qkv_bias_all = biases[:, None, :edge_out]
    up_bias_all = biases[:, edge_out:]

    tokens_in = to_sequence(inputs).astype(F32)
    ids = to_sequence(image_ids)
    grad_low = to_sequence(cotangent)
    grad_y = grad_low.astype(F32)

    unit_one, scaled_one = norm_parts(tokens_in)
    normed1 = (unit_one * norm1_gain + norm1_bias).astype(BF)
    project, mixed = attend(
        normed1, gathered, qkv_bias_all, query_gain, query_bias, key_gain, ids, local_width
    )
    resid = tokens_in + out_bias
    for i in range(tp):
        resid = resid + mm_nt(mixed[:, i * local_width : (i + 1) * local_width], out_t[i])
    unit_two, scaled_two = norm_parts(resid)
    normed2 = (unit_two * norm2_gain + norm2_bias).astype(BF)

    output = resid + down_bias
    hidden, slope = [], []
    for i in range(tp):
        preact = mm(normed2, up[i]) + up_bias_all[i]
        half = 0.5 * (1.0 + lax.erf(preact * (0.5**0.5)))
        bell = jnp.exp(-0.5 * preact * preact) * ((0.5 / jnp.pi) ** 0.5)
        hidden.append((preact * half).astype(BF))
        slope.append((half + preact * bell).astype(BF))
        output = output + mm_nt(hidden[i], down_t[i])
    output = from_sequence(output.astype(BF), BF)

    grad_normed2 = 0.0
    terms_up, terms_down, sums_up = [], [], []
    for i in range(tp):
        grad_preact = (mm(grad_low, down_t[i]) * slope[i].astype(F32)).astype(BF)
        grad_normed2 = grad_normed2 + mm_nt(grad_preact, up[i])
        terms_up.append(mm_tn(normed2, grad_preact).astype(BF))
        terms_down.append(mm_tn(grad_low, hidden[i]).astype(BF))
        sums_up.append(jnp.sum(grad_preact.astype(F32), axis=0))
    late = jnp.stack(
        [jnp.concatenate([terms_up[i], terms_down[i]], axis=1) for i in range(tp)]
    ).reshape(tp * width, -1)
    late = lax.psum_scatter(late, everyone, scatter_dimension=0, tiled=True).astype(F32)
    up_weight_grad = late[:, :local_hidden]
    down_weight_grad = late[:, local_hidden:].T

    grad_resid = grad_y + norm_back(grad_normed2, unit_two, scaled_two, norm2_gain)
    grad_resr = grad_resid.astype(BF)
    grad_project, head_sums = attend_back(
        grad_resr,
        gathered,
        edge_out,
        project,
        query_gain,
        query_bias,
        key_gain,
        ids,
        local_width,
    )
    grad_normed1 = 0.0
    terms_qkv, terms_out, sums_qkv = [], [], []
    for i in range(tp):
        grad_normed1 = grad_normed1 + mm_nt(grad_project[i], qkv[i])
        terms_qkv.append(mm_tn(normed1, grad_project[i]).astype(BF))
        terms_out.append(
            mm_tn(grad_resr, mixed[:, i * local_width : (i + 1) * local_width]).astype(BF)
        )
        sums_qkv.append(jnp.sum(grad_project[i].astype(F32), axis=0))
    early = jnp.stack(
        [jnp.concatenate([terms_qkv[i], terms_out[i]], axis=1) for i in range(tp)]
    ).reshape(tp * width, -1)
    early = lax.psum_scatter(early, everyone, scatter_dimension=0, tiled=True).astype(F32)
    qkv_weight_grad = (
        early[:, :edge_out]
        .reshape(shard, per, 3, lanes)
        .transpose(0, 2, 1, 3)
        .reshape(qkv_weight.shape)
    )
    out_weight_grad = early[:, edge_out:].T

    input_grad = grad_resid + norm_back(grad_normed1, unit_one, scaled_one, norm1_gain)
    input_grad = from_sequence(input_grad, BF)

    vectors = [
        jnp.sum(grad_normed1 * unit_one, axis=0),
        jnp.sum(grad_normed1, axis=0),
        head_sums[0],
        head_sums[1],
        head_sums[2],
        jnp.sum(grad_resid, axis=0),
        jnp.sum(grad_normed2 * unit_two, axis=0),
        jnp.sum(grad_normed2, axis=0),
        jnp.sum(grad_y, axis=0),
        *sums_qkv,
        *sums_up,
    ]
    summed = lax.psum(jnp.concatenate(vectors), everyone)
    pieces, start = [], 0
    for vector in vectors:
        pieces.append(summed[start : start + vector.shape[0]])
        start += vector.shape[0]
    gain_one, shift_one, gain_query, shift_query, gain_key = pieces[:5]
    sum_out, gain_two, shift_two, sum_down = pieces[5:9]
    qkv_bias_grad = jnp.where(me == 0, pieces[9], pieces[10])
    qkv_bias_grad = qkv_bias_grad.reshape(per, 3, lanes).transpose(1, 0, 2).reshape(qkv_bias.shape)
    up_bias_grad = jnp.where(me == 0, pieces[11], pieces[12])
    return (
        output,
        input_grad,
        gain_one,
        shift_one,
        qkv_weight_grad,
        qkv_bias_grad,
        gain_query,
        shift_query,
        gain_key,
        out_weight_grad,
        sum_out,
        gain_two,
        shift_two,
        up_weight_grad,
        up_bias_grad,
        down_weight_grad,
        sum_down,
    )


def solution(mesh):
    placed = (
        P(None, ("fsdp", "tp"), None),
        P(None, ("fsdp", "tp")),
        P(None, ("fsdp", "tp"), None),
        P(),
        P(),
        P("fsdp", None, "tp"),
        P(None, "tp"),
        P(),
        P(),
        P(),
        P("tp", "fsdp"),
        P(),
        P(),
        P(),
        P("fsdp", "tp"),
        P("tp"),
        P("tp", "fsdp"),
        P(),
    )
    return jax.shard_map(
        on_device,
        mesh=mesh,
        in_specs=placed,
        out_specs=(
            P(None, ("fsdp", "tp"), None),
            P(None, ("fsdp", "tp"), None),
            P(),
            P(),
            P("fsdp", None, "tp"),
            P(None, "tp"),
            P(),
            P(),
            P(),
            P("tp", "fsdp"),
            P(),
            P(),
            P(),
            P("fsdp", "tp"),
            P("tp"),
            P("tp", "fsdp"),
            P(),
        ),
        check_vma=False,
    )
```

```python
from functools import partial

import jax
import jax.numpy as jnp
from jax import lax
from jax.experimental import pallas as pl
from jax.experimental.pallas import tpu as pltpu
from jax.sharding import PartitionSpec as P

LEN = 1024
IMG_MOST = 256
BLOCK = 256
REACH = -(-(IMG_MOST - 1) // BLOCK)
EPSILON = 1e-06
BF = jnp.bfloat16
F32 = jnp.float32


def norm_parts(values):
    average = jnp.mean(values, axis=-1, keepdims=True)
    centred = values - average
    spread = jnp.mean(centred * centred, axis=-1, keepdims=True)
    scaled = lax.rsqrt(spread + EPSILON)
    return (centred * scaled, scaled)


def norm_back(grad_out, unit, scaled, gain):
    grad_unit = grad_out * gain
    first = jnp.mean(grad_unit, axis=-1, keepdims=True)
    second = jnp.mean(grad_unit * unit, axis=-1, keepdims=True)
    return scaled * (grad_unit - first - unit * second)


def mm(a, b):
    return jnp.dot(a, b, preferred_element_type=F32)


def mm_nt(a, b):
    return lax.dot_general(a, b, (((1,), (1,)), ((), ())), preferred_element_type=F32)


def mm_tn(a, b):
    return lax.dot_general(a, b, (((0,), (0,)), ((), ())), preferred_element_type=F32)


def key_range(block, count):
    return max(0, block - REACH), min(count, block + REACH + 1)


def attend_kernel(
    x_ref, w_ref, b_ref, qg_ref, qb_ref, kg_ref, idc_ref, idr_ref, p_ref, mixed_ref, *, depth
):
    length = x_ref.shape[0]
    lanes = mixed_ref.shape[1]
    count = length // BLOCK
    scale = depth ** (-0.5)
    project = mm(x_ref[...], w_ref[0]) + b_ref[0]
    p_ref[0] = project
    heads = []
    for head in range(lanes // depth):
        part = [
            project[:, i * lanes + head * depth : i * lanes + (head + 1) * depth] for i in range(3)
        ]
        query = (norm_parts(part[0])[0] * qg_ref[...] + qb_ref[...]).astype(BF)
        query = query * jnp.asarray(scale, BF)
        key = (norm_parts(part[1])[0] * kg_ref[...]).astype(BF)
        value = part[2].astype(BF)
        value = jnp.concatenate([value, jnp.ones_like(value)], axis=1)
        rows = []
        for block in range(count):
            low, high = key_range(block, count)
            q = slice(block * BLOCK, (block + 1) * BLOCK)
            k = slice(low * BLOCK, high * BLOCK)
            scores = mm_nt(query[q], key[k])
            same = idc_ref[q, :] == idr_ref[:, k]
            weights = jnp.where(same, jnp.exp(scores), 0.0).astype(BF)
            both = mm(weights, value[k])
            rows.append(both[:, :depth] / both[:, depth : depth + 1])
        heads.append(jnp.concatenate(rows, axis=0))
    mixed_ref[...] = jnp.concatenate(heads, axis=1).astype(BF)


def attend_back_kernel(
    g_ref, w_ref, p_ref, qg_ref, qb_ref, kg_ref, idc_ref, idr_ref, gp_ref, sums_ref, *, depth
):
    length = g_ref.shape[0]
    lanes = w_ref.shape[2]
    count = length // BLOCK
    scale = depth ** (-0.5)
    grad_mixed = mm(g_ref[...], w_ref[0]).astype(BF)
    project = p_ref[0]
    sums = [jnp.zeros((1, depth), F32) for _ in range(3)]
    columns = [[], [], []]
    for head in range(lanes // depth):
        part = [
            project[:, i * lanes + head * depth : i * lanes + (head + 1) * depth] for i in range(3)
        ]
        query_unit, query_scaled = norm_parts(part[0])
        key_unit, key_scaled = norm_parts(part[1])
        query = (query_unit * qg_ref[...] + qb_ref[...]).astype(BF)
        query = query * jnp.asarray(scale, BF)
        key = (key_unit * kg_ref[...]).astype(BF)
        value = part[2].astype(BF)
        grad = grad_mixed[:, head * depth : (head + 1) * depth]
        grad_key = [None] * count
        grad_value = [None] * count
        grad_query = []
        for block in range(count):
            low, high = key_range(block, count)
            q = slice(block * BLOCK, (block + 1) * BLOCK)
            k = slice(low * BLOCK, high * BLOCK)
            scores = mm_nt(key[k], query[q])
            same = idc_ref[k, :] == idr_ref[:, q]
            raised = jnp.where(same, jnp.exp(scores), 0.0)
            weights = raised * (1.0 / jnp.sum(raised, axis=0, keepdims=True))
            grad_weights = mm_nt(value[k], grad[q])
            inner = jnp.sum(grad_weights * weights, axis=0, keepdims=True)
            grad_scores = (weights * (grad_weights - inner)).astype(BF)
            grad_query.append(mm_tn(grad_scores, key[k]) * scale)
            to_key = mm(grad_scores, query[q])
            to_value = mm(weights.astype(BF), grad[q])
            for i in range(low, high):
                piece = slice((i - low) * BLOCK, (i - low + 1) * BLOCK)
                grad_key[i] = to_key[piece] if grad_key[i] is None else grad_key[i] + to_key[piece]
                grad_value[i] = (
                    to_value[piece] if grad_value[i] is None else grad_value[i] + to_value[piece]
                )
        grad_query = jnp.concatenate(grad_query, axis=0)
        grad_key = jnp.concatenate(grad_key, axis=0)
        grad_value = jnp.concatenate(grad_value, axis=0)
        sums[0] += jnp.sum(grad_query * query_unit, axis=0, keepdims=True)
        sums[1] += jnp.sum(grad_query, axis=0, keepdims=True)
        sums[2] += jnp.sum(grad_key * key_unit, axis=0, keepdims=True)
        columns[0].append(norm_back(grad_query, query_unit, query_scaled, qg_ref[...]))
        columns[1].append(norm_back(grad_key, key_unit, key_scaled, kg_ref[...]))
        columns[2].append(grad_value)
    for i in range(3):
        gp_ref[0, :, i * lanes : (i + 1) * lanes] = jnp.concatenate(columns[i], axis=1).astype(BF)

    @pl.when(pl.program_id(0) == 0)
    def _():
        sums_ref[...] = jnp.zeros_like(sums_ref)

    for i in range(3):
        sums_ref[i : i + 1, :] += sums[i]


def sum_by_pairs(vector, axes):
    for axis in axes:
        size = lax.axis_size(axis)
        assert size & (size - 1) == 0
        step = 1
        while step < size:
            vector = vector + lax.ppermute(vector, axis, [(i, i ^ step) for i in range(size)])
            step *= 2
    return vector


def attend(normed, weight, bias, query_gain, query_bias, key_gain, ids, local_width):
    length, width = normed.shape
    tp = weight.shape[0]
    depth = query_gain.shape[0]
    lanes = 2 * depth
    per = local_width // lanes
    whole = lambda *shape: pl.BlockSpec(shape, lambda i: (0,) * len(shape))
    return pl.pallas_call(
        partial(attend_kernel, depth=depth),
        grid=(tp * per,),
        in_specs=[
            whole(length, width),
            pl.BlockSpec((1, width, 3 * lanes), lambda i: (i // per, 0, i % per)),
            pl.BlockSpec((1, 1, 3 * lanes), lambda i: (i // per, 0, i % per)),
            whole(1, depth),
            whole(1, depth),
            whole(1, depth),
            whole(length, 1),
            whole(1, length),
        ],
        out_specs=[
            pl.BlockSpec((1, length, 3 * lanes), lambda i: (i // per, 0, i % per)),
            pl.BlockSpec((length, lanes), lambda i: (0, i)),
        ],
        out_shape=[
            jax.ShapeDtypeStruct((tp, length, 3 * local_width), F32),
            jax.ShapeDtypeStruct((length, tp * local_width), BF),
        ],
        compiler_params=pltpu.CompilerParams(vmem_limit_bytes=56 * 2**20),
        cost_estimate=pl.CostEstimate(
            flops=2 * length * width * 3 * local_width * tp,
            bytes_accessed=length * local_width * tp * 16,
            transcendentals=length * 3 * BLOCK * tp * local_width // depth,
        ),
        name="attend",
    )(
        normed,
        weight,
        bias,
        query_gain[None],
        query_bias[None],
        key_gain[None],
        ids[:, None],
        ids[None],
    )


def attend_back(
    grad_rows, weight, out_column, project, query_gain, query_bias, key_gain, ids, local_width
):
    length, width = grad_rows.shape
    tp = weight.shape[0]
    depth = query_gain.shape[0]
    lanes = 2 * depth
    per = local_width // lanes
    first = out_column // lanes
    whole = lambda *shape: pl.BlockSpec(shape, lambda i: (0,) * len(shape))
    return pl.pallas_call(
        partial(attend_back_kernel, depth=depth),
        grid=(tp * per,),
        in_specs=[
            whole(length, width),
            pl.BlockSpec((1, width, lanes), lambda i: (i // per, 0, first + i % per)),
            pl.BlockSpec((1, length, 3 * lanes), lambda i: (i // per, 0, i % per)),
            whole(1, depth),
            whole(1, depth),
            whole(1, depth),
            whole(length, 1),
            whole(1, length),
        ],
        out_specs=[
            pl.BlockSpec((1, length, 3 * lanes), lambda i: (i // per, 0, i % per)),
            whole(3, depth),
        ],
        out_shape=[
            jax.ShapeDtypeStruct((tp, length, 3 * local_width), BF),
            jax.ShapeDtypeStruct((3, depth), F32),
        ],
        compiler_params=pltpu.CompilerParams(vmem_limit_bytes=56 * 2**20),
        cost_estimate=pl.CostEstimate(
            flops=8 * length * width * local_width * tp,
            bytes_accessed=length * local_width * tp * 18,
            transcendentals=length * 3 * BLOCK * tp * local_width // depth,
        ),
        name="attend_back",
    )(
        grad_rows,
        weight,
        project,
        query_gain[None],
        query_bias[None],
        key_gain[None],
        ids[:, None],
        ids[None],
    )


def on_device(
    inputs,
    image_ids,
    cotangent,
    norm1_gain,
    norm1_bias,
    qkv_weight,
    qkv_bias,
    query_gain,
    query_bias,
    key_gain,
    out_weight,
    out_bias,
    norm2_gain,
    norm2_bias,
    up_weight,
    up_bias,
    down_weight,
    down_bias,
):
    batches, rows_here, width = inputs.shape
    tp = lax.axis_size("tp")
    me = lax.axis_index("tp")
    assert batches == 2 and tp == 2 and rows_here * tp == LEN
    everyone = ("tp", "fsdp")
    shard = qkv_weight.shape[0]
    local_width = qkv_weight.shape[2]
    local_hidden = up_weight.shape[1]
    lanes = 2 * query_gain.shape[0]
    per = local_width // lanes
    swap = [(0, 1), (1, 0)]

    def pick(array, index):
        return lax.dynamic_index_in_dim(array, index, 0, keepdims=False)

    def in_order(own, other):
        return jnp.where(
            me == 0, jnp.concatenate([own, other], 0), jnp.concatenate([other, own], 0)
        )

    def to_sequence(array):
        return in_order(pick(array, me), lax.ppermute(pick(array, 1 - me), "tp", swap))

    def from_sequence(array, dtype):
        halves = array.reshape(2, rows_here, width)
        other = lax.ppermute(pick(halves, 1 - me).astype(dtype), "tp", swap).astype(array.dtype)
        own = pick(halves, me)
        return jnp.where(me == 0, jnp.stack([own, other]), jnp.stack([other, own]))

    packed = jnp.concatenate(
        [
            qkv_weight.reshape(shard, 3, per, lanes).transpose(0, 2, 1, 3).reshape(shard, -1),
            out_weight.T,
            up_weight,
            down_weight.T,
        ],
        axis=1,
    )
    gathered = lax.all_gather(packed, everyone, axis=0, tiled=True).reshape(tp, width, -1)
    edge_out = 3 * local_width
    edge_up = edge_out + local_width
    edge_down = edge_up + local_hidden
    out_t = [gathered[i, :, edge_out:edge_up] for i in range(tp)]
    up = [gathered[i, :, edge_up:edge_down] for i in range(tp)]
    down_t = [gathered[i, :, edge_down:] for i in range(tp)]
    qkv = [gathered[i, :, :edge_out] for i in range(tp)]

    biases = jnp.concatenate(
        [qkv_bias.reshape(3, per, lanes).transpose(1, 0, 2).reshape(-1), up_bias]
    )
    biases = in_order(biases[None], lax.ppermute(biases, "tp", swap)[None])
    qkv_bias_all = biases[:, None, :edge_out]
    up_bias_all = biases[:, edge_out:]

    tokens_in = to_sequence(inputs).astype(F32)
    ids = to_sequence(image_ids)
    grad_low = to_sequence(cotangent)
    grad_y = grad_low.astype(F32)

    unit_one, scaled_one = norm_parts(tokens_in)
    normed1 = (unit_one * norm1_gain + norm1_bias).astype(BF)
    project, mixed = attend(
        normed1, gathered, qkv_bias_all, query_gain, query_bias, key_gain, ids, local_width
    )
    resid = tokens_in + out_bias
    for i in range(tp):
        resid = resid + mm_nt(mixed[:, i * local_width : (i + 1) * local_width], out_t[i])
    unit_two, scaled_two = norm_parts(resid)
    normed2 = (unit_two * norm2_gain + norm2_bias).astype(BF)

    output = resid + down_bias
    hidden, slope = [], []
    for i in range(tp):
        preact = mm(normed2, up[i]) + up_bias_all[i]
        half = 0.5 * (1.0 + lax.erf(preact * (0.5**0.5)))
        bell = jnp.exp(-0.5 * preact * preact) * ((0.5 / jnp.pi) ** 0.5)
        hidden.append((preact * half).astype(BF))
        slope.append((half + preact * bell).astype(BF))
        output = output + mm_nt(hidden[i], down_t[i])
    output = from_sequence(output.astype(BF), BF)

    grad_normed2 = 0.0
    terms_up, terms_down, sums_up = [], [], []
    for i in range(tp):
        grad_preact = (mm(grad_low, down_t[i]) * slope[i].astype(F32)).astype(BF)
        grad_normed2 = grad_normed2 + mm_nt(grad_preact, up[i])
        terms_up.append(mm_tn(normed2, grad_preact).astype(BF))
        terms_down.append(mm_tn(grad_low, hidden[i]).astype(BF))
        sums_up.append(jnp.sum(grad_preact.astype(F32), axis=0))
    grad_resid = grad_y + norm_back(grad_normed2, unit_two, scaled_two, norm2_gain)
    grad_resr = grad_resid.astype(BF)
    terms_out = [
        mm_tn(grad_resr, mixed[:, i * local_width : (i + 1) * local_width]).astype(BF)
        for i in range(tp)
    ]
    late = jnp.stack(
        [jnp.concatenate([terms_up[i], terms_down[i], terms_out[i]], axis=1) for i in range(tp)]
    ).reshape(tp * width, -1)
    late, grad_resr = lax.optimization_barrier((late, grad_resr))
    late = lax.psum_scatter(late, everyone, scatter_dimension=0, tiled=True)
    late = late.astype(F32)
    up_weight_grad = late[:, :local_hidden]
    down_weight_grad = late[:, local_hidden : 2 * local_hidden].T
    out_weight_grad = late[:, 2 * local_hidden :].T

    grad_project, head_sums = attend_back(
        grad_resr,
        gathered,
        edge_out,
        project,
        query_gain,
        query_bias,
        key_gain,
        ids,
        local_width,
    )
    grad_normed1 = 0.0
    terms_qkv, sums_qkv = [], []
    for i in range(tp):
        terms_qkv.append(mm_tn(normed1, grad_project[i]).astype(BF))
        sums_qkv.append(jnp.sum(grad_project[i].astype(F32), axis=0))
    early = jnp.stack(terms_qkv)
    early, grad_project = lax.optimization_barrier((early, grad_project))
    theirs = lax.ppermute(pick(early, 1 - me), "tp", swap)
    early = (pick(early, me).astype(F32) + theirs.astype(F32)).astype(BF)
    early = lax.psum_scatter(early, "fsdp", scatter_dimension=0, tiled=True).astype(F32)
    for i in range(tp):
        grad_normed1 = grad_normed1 + mm_nt(grad_project[i], qkv[i])
    qkv_weight_grad = (
        early.reshape(shard, per, 3, lanes)
        .transpose(0, 2, 1, 3)
        .reshape(qkv_weight.shape)
    )
    input_grad = grad_resid + norm_back(grad_normed1, unit_one, scaled_one, norm1_gain)
    input_grad = from_sequence(input_grad, BF)

    vectors = [
        jnp.sum(grad_normed1 * unit_one, axis=0),
        jnp.sum(grad_normed1, axis=0),
        head_sums[0],
        head_sums[1],
        head_sums[2],
        jnp.sum(grad_resid, axis=0),
        jnp.sum(grad_normed2 * unit_two, axis=0),
        jnp.sum(grad_normed2, axis=0),
        jnp.sum(grad_y, axis=0),
        *sums_qkv,
        *sums_up,
    ]
    summed = sum_by_pairs(jnp.concatenate(vectors), everyone)
    pieces, start = [], 0
    for vector in vectors:
        pieces.append(summed[start : start + vector.shape[0]])
        start += vector.shape[0]
    gain_one, shift_one, gain_query, shift_query, gain_key = pieces[:5]
    sum_out, gain_two, shift_two, sum_down = pieces[5:9]
    qkv_bias_grad = jnp.where(me == 0, pieces[9], pieces[10])
    qkv_bias_grad = qkv_bias_grad.reshape(per, 3, lanes).transpose(1, 0, 2).reshape(qkv_bias.shape)
    up_bias_grad = jnp.where(me == 0, pieces[11], pieces[12])
    return (
        output,
        input_grad,
        gain_one,
        shift_one,
        qkv_weight_grad,
        qkv_bias_grad,
        gain_query,
        shift_query,
        gain_key,
        out_weight_grad,
        sum_out,
        gain_two,
        shift_two,
        up_weight_grad,
        up_bias_grad,
        down_weight_grad,
        sum_down,
    )


def solution(mesh):
    placed = (
        P(None, ("fsdp", "tp"), None),
        P(None, ("fsdp", "tp")),
        P(None, ("fsdp", "tp"), None),
        P(),
        P(),
        P("fsdp", None, "tp"),
        P(None, "tp"),
        P(),
        P(),
        P(),
        P("tp", "fsdp"),
        P(),
        P(),
        P(),
        P("fsdp", "tp"),
        P("tp"),
        P("tp", "fsdp"),
        P(),
    )
    return jax.shard_map(
        on_device,
        mesh=mesh,
        in_specs=placed,
        out_specs=(
            P(None, ("fsdp", "tp"), None),
            P(None, ("fsdp", "tp"), None),
            P(),
            P(),
            P("fsdp", None, "tp"),
            P(None, "tp"),
            P(),
            P(),
            P(),
            P("tp", "fsdp"),
            P(),
            P(),
            P(),
            P("fsdp", "tp"),
            P("tp"),
            P("tp", "fsdp"),
            P(),
        ),
        check_vma=False,
    )
```

```python
from functools import partial

import jax
import jax.numpy as jnp
from jax import lax
from jax.experimental import pallas as pl
from jax.experimental.pallas import tpu as pltpu
from jax.sharding import PartitionSpec as P

LEN = 1024
IMG_MOST = 256
BLOCK = 256
REACH = -(-(IMG_MOST - 1) // BLOCK)
EPSILON = 1e-06
BF = jnp.bfloat16
F32 = jnp.float32


def norm_parts(values):
    average = jnp.mean(values, axis=-1, keepdims=True)
    centred = values - average
    spread = jnp.mean(centred * centred, axis=-1, keepdims=True)
    scaled = lax.rsqrt(spread + EPSILON)
    return (centred * scaled, scaled)


def norm_back(grad_out, unit, scaled, gain):
    grad_unit = grad_out * gain
    first = jnp.mean(grad_unit, axis=-1, keepdims=True)
    second = jnp.mean(grad_unit * unit, axis=-1, keepdims=True)
    return scaled * (grad_unit - first - unit * second)


def mm(a, b):
    return jnp.dot(a, b, preferred_element_type=F32)


def mm_nt(a, b):
    return lax.dot_general(a, b, (((1,), (1,)), ((), ())), preferred_element_type=F32)


def mm_tn(a, b):
    return lax.dot_general(a, b, (((0,), (0,)), ((), ())), preferred_element_type=F32)


def key_range(block, count):
    return max(0, block - REACH), min(count, block + REACH + 1)


def attend_kernel(
    x_ref, w_ref, b_ref, qg_ref, qb_ref, kg_ref, idc_ref, idr_ref, p_ref, mixed_ref, *, depth
):
    length = x_ref.shape[0]
    lanes = mixed_ref.shape[1]
    count = length // BLOCK
    scale = depth ** (-0.5)
    project = mm(x_ref[...], w_ref[0]) + b_ref[0]
    p_ref[0] = project
    heads = []
    for head in range(lanes // depth):
        part = [
            project[:, i * lanes + head * depth : i * lanes + (head + 1) * depth] for i in range(3)
        ]
        query = (norm_parts(part[0])[0] * qg_ref[...] + qb_ref[...]).astype(BF)
        query = query * jnp.asarray(scale, BF)
        key = (norm_parts(part[1])[0] * kg_ref[...]).astype(BF)
        value = part[2].astype(BF)
        value = jnp.concatenate([value, jnp.ones_like(value)], axis=1)
        rows = []
        for block in range(count):
            low, high = key_range(block, count)
            q = slice(block * BLOCK, (block + 1) * BLOCK)
            k = slice(low * BLOCK, high * BLOCK)
            scores = mm_nt(query[q], key[k])
            same = idc_ref[q, :] == idr_ref[:, k]
            weights = jnp.where(same, jnp.exp(scores), 0.0).astype(BF)
            both = mm(weights, value[k])
            rows.append(both[:, :depth] / both[:, depth : depth + 1])
        heads.append(jnp.concatenate(rows, axis=0))
    mixed_ref[...] = jnp.concatenate(heads, axis=1).astype(BF)


def attend_back_kernel(
    g_ref, w_ref, p_ref, qg_ref, qb_ref, kg_ref, idc_ref, idr_ref, gp_ref, sums_ref, *, depth
):
    length = g_ref.shape[0]
    lanes = w_ref.shape[2]
    count = length // BLOCK
    scale = depth ** (-0.5)
    grad_mixed = mm(g_ref[...], w_ref[0]).astype(BF)
    project = p_ref[0]
    sums = [jnp.zeros((1, depth), F32) for _ in range(3)]
    columns = [[], [], []]
    for head in range(lanes // depth):
        part = [
            project[:, i * lanes + head * depth : i * lanes + (head + 1) * depth] for i in range(3)
        ]
        query_unit, query_scaled = norm_parts(part[0])
        key_unit, key_scaled = norm_parts(part[1])
        query = (query_unit * qg_ref[...] + qb_ref[...]).astype(BF)
        query = query * jnp.asarray(scale, BF)
        key = (key_unit * kg_ref[...]).astype(BF)
        value = part[2].astype(BF)
        grad = grad_mixed[:, head * depth : (head + 1) * depth]
        grad_key = [None] * count
        grad_value = [None] * count
        grad_query = []
        for block in range(count):
            low, high = key_range(block, count)
            q = slice(block * BLOCK, (block + 1) * BLOCK)
            k = slice(low * BLOCK, high * BLOCK)
            scores = mm_nt(key[k], query[q])
            same = idc_ref[k, :] == idr_ref[:, q]
            raised = jnp.where(same, jnp.exp(scores), 0.0)
            weights = raised * (1.0 / jnp.sum(raised, axis=0, keepdims=True))
            grad_weights = mm_nt(value[k], grad[q])
            inner = jnp.sum(grad_weights * weights, axis=0, keepdims=True)
            grad_scores = (weights * (grad_weights - inner)).astype(BF)
            grad_query.append(mm_tn(grad_scores, key[k]) * scale)
            to_key = mm(grad_scores, query[q])
            to_value = mm(weights.astype(BF), grad[q])
            for i in range(low, high):
                piece = slice((i - low) * BLOCK, (i - low + 1) * BLOCK)
                grad_key[i] = to_key[piece] if grad_key[i] is None else grad_key[i] + to_key[piece]
                grad_value[i] = (
                    to_value[piece] if grad_value[i] is None else grad_value[i] + to_value[piece]
                )
        grad_query = jnp.concatenate(grad_query, axis=0)
        grad_key = jnp.concatenate(grad_key, axis=0)
        grad_value = jnp.concatenate(grad_value, axis=0)
        sums[0] += jnp.sum(grad_query * query_unit, axis=0, keepdims=True)
        sums[1] += jnp.sum(grad_query, axis=0, keepdims=True)
        sums[2] += jnp.sum(grad_key * key_unit, axis=0, keepdims=True)
        columns[0].append(norm_back(grad_query, query_unit, query_scaled, qg_ref[...]))
        columns[1].append(norm_back(grad_key, key_unit, key_scaled, kg_ref[...]))
        columns[2].append(grad_value)
    for i in range(3):
        gp_ref[0, :, i * lanes : (i + 1) * lanes] = jnp.concatenate(columns[i], axis=1).astype(BF)

    @pl.when(pl.program_id(0) == 0)
    def _():
        sums_ref[...] = jnp.zeros_like(sums_ref)

    for i in range(3):
        sums_ref[i : i + 1, :] += sums[i]


def add_halves(own, other):
    return (own.astype(F32) + other.astype(F32)).astype(BF)


def halve_over_fsdp(array, step):
    size = lax.axis_size("fsdp")
    assert size & (size - 1) == 0
    bit = lax.axis_index("fsdp") // step % 2
    pairs = array.reshape(array.shape[0], -1, 2, *array.shape[2:])
    own = lax.dynamic_index_in_dim(pairs, bit, 2, keepdims=False)
    other = lax.dynamic_index_in_dim(pairs, 1 - bit, 2, keepdims=False)
    return add_halves(own, lax.ppermute(other, "fsdp", [(i, i ^ step) for i in range(size)]))


def sum_by_pairs(vector, axes):
    for axis in axes:
        size = lax.axis_size(axis)
        assert size & (size - 1) == 0
        step = 1
        while step < size:
            vector = vector + lax.ppermute(vector, axis, [(i, i ^ step) for i in range(size)])
            step *= 2
    return vector


def attend(normed, weight, bias, query_gain, query_bias, key_gain, ids, local_width):
    length, width = normed.shape
    tp = weight.shape[0]
    depth = query_gain.shape[0]
    lanes = 2 * depth
    per = local_width // lanes
    whole = lambda *shape: pl.BlockSpec(shape, lambda i: (0,) * len(shape))
    return pl.pallas_call(
        partial(attend_kernel, depth=depth),
        grid=(tp * per,),
        in_specs=[
            whole(length, width),
            pl.BlockSpec((1, width, 3 * lanes), lambda i: (i // per, 0, i % per)),
            pl.BlockSpec((1, 1, 3 * lanes), lambda i: (i // per, 0, i % per)),
            whole(1, depth),
            whole(1, depth),
            whole(1, depth),
            whole(length, 1),
            whole(1, length),
        ],
        out_specs=[
            pl.BlockSpec((1, length, 3 * lanes), lambda i: (i // per, 0, i % per)),
            pl.BlockSpec((length, lanes), lambda i: (0, i)),
        ],
        out_shape=[
            jax.ShapeDtypeStruct((tp, length, 3 * local_width), F32),
            jax.ShapeDtypeStruct((length, tp * local_width), BF),
        ],
        compiler_params=pltpu.CompilerParams(vmem_limit_bytes=56 * 2**20),
        cost_estimate=pl.CostEstimate(
            flops=2 * length * width * 3 * local_width * tp,
            bytes_accessed=length * local_width * tp * 16,
            transcendentals=length * 3 * BLOCK * tp * local_width // depth,
        ),
        name="attend",
    )(
        normed,
        weight,
        bias,
        query_gain[None],
        query_bias[None],
        key_gain[None],
        ids[:, None],
        ids[None],
    )


def attend_back(
    grad_rows, weight, out_column, project, query_gain, query_bias, key_gain, ids, local_width
):
    length, width = grad_rows.shape
    tp = weight.shape[0]
    depth = query_gain.shape[0]
    lanes = 2 * depth
    per = local_width // lanes
    first = out_column // lanes
    whole = lambda *shape: pl.BlockSpec(shape, lambda i: (0,) * len(shape))
    return pl.pallas_call(
        partial(attend_back_kernel, depth=depth),
        grid=(tp * per,),
        in_specs=[
            whole(length, width),
            pl.BlockSpec((1, width, lanes), lambda i: (i // per, 0, first + i % per)),
            pl.BlockSpec((1, length, 3 * lanes), lambda i: (i // per, 0, i % per)),
            whole(1, depth),
            whole(1, depth),
            whole(1, depth),
            whole(length, 1),
            whole(1, length),
        ],
        out_specs=[
            pl.BlockSpec((1, length, 3 * lanes), lambda i: (i // per, 0, i % per)),
            whole(3, depth),
        ],
        out_shape=[
            jax.ShapeDtypeStruct((tp, length, 3 * local_width), BF),
            jax.ShapeDtypeStruct((3, depth), F32),
        ],
        compiler_params=pltpu.CompilerParams(vmem_limit_bytes=56 * 2**20),
        cost_estimate=pl.CostEstimate(
            flops=8 * length * width * local_width * tp,
            bytes_accessed=length * local_width * tp * 18,
            transcendentals=length * 3 * BLOCK * tp * local_width // depth,
        ),
        name="attend_back",
    )(
        grad_rows,
        weight,
        project,
        query_gain[None],
        query_bias[None],
        key_gain[None],
        ids[:, None],
        ids[None],
    )


def on_device(
    inputs,
    image_ids,
    cotangent,
    norm1_gain,
    norm1_bias,
    qkv_weight,
    qkv_bias,
    query_gain,
    query_bias,
    key_gain,
    out_weight,
    out_bias,
    norm2_gain,
    norm2_bias,
    up_weight,
    up_bias,
    down_weight,
    down_bias,
):
    batches, rows_here, width = inputs.shape
    tp = lax.axis_size("tp")
    me = lax.axis_index("tp")
    assert batches == 2 and tp == 2 and rows_here * tp == LEN
    everyone = ("tp", "fsdp")
    shard = qkv_weight.shape[0]
    local_width = qkv_weight.shape[2]
    local_hidden = up_weight.shape[1]
    lanes = 2 * query_gain.shape[0]
    per = local_width // lanes
    swap = [(0, 1), (1, 0)]

    def pick(array, index):
        return lax.dynamic_index_in_dim(array, index, 0, keepdims=False)

    def in_order(own, other):
        return jnp.where(
            me == 0, jnp.concatenate([own, other], 0), jnp.concatenate([other, own], 0)
        )

    def to_sequence(array):
        return in_order(pick(array, me), lax.ppermute(pick(array, 1 - me), "tp", swap))

    def from_sequence(array, dtype):
        halves = array.reshape(2, rows_here, width)
        other = lax.ppermute(pick(halves, 1 - me).astype(dtype), "tp", swap).astype(array.dtype)
        own = pick(halves, me)
        return jnp.where(me == 0, jnp.stack([own, other]), jnp.stack([other, own]))

    packed = jnp.concatenate(
        [
            qkv_weight.reshape(shard, 3, per, lanes).transpose(0, 2, 1, 3).reshape(shard, -1),
            out_weight.T,
            up_weight,
            down_weight.T,
        ],
        axis=1,
    )
    gathered = lax.all_gather(packed, everyone, axis=0, tiled=True).reshape(tp, width, -1)
    edge_out = 3 * local_width
    edge_up = edge_out + local_width
    edge_down = edge_up + local_hidden
    out_t = [gathered[i, :, edge_out:edge_up] for i in range(tp)]
    up = [gathered[i, :, edge_up:edge_down] for i in range(tp)]
    down_t = [gathered[i, :, edge_down:] for i in range(tp)]
    qkv = [gathered[i, :, :edge_out] for i in range(tp)]

    biases = jnp.concatenate(
        [qkv_bias.reshape(3, per, lanes).transpose(1, 0, 2).reshape(-1), up_bias]
    )
    biases = in_order(biases[None], lax.ppermute(biases, "tp", swap)[None])
    qkv_bias_all = biases[:, None, :edge_out]
    up_bias_all = biases[:, edge_out:]

    tokens_in = to_sequence(inputs).astype(F32)
    ids = to_sequence(image_ids)
    grad_low = to_sequence(cotangent)
    grad_y = grad_low.astype(F32)

    unit_one, scaled_one = norm_parts(tokens_in)
    normed1 = (unit_one * norm1_gain + norm1_bias).astype(BF)
    project, mixed = attend(
        normed1, gathered, qkv_bias_all, query_gain, query_bias, key_gain, ids, local_width
    )
    resid = tokens_in + out_bias
    for i in range(tp):
        resid = resid + mm_nt(mixed[:, i * local_width : (i + 1) * local_width], out_t[i])
    unit_two, scaled_two = norm_parts(resid)
    normed2 = (unit_two * norm2_gain + norm2_bias).astype(BF)

    hidden, slope = [], []
    for i in range(tp):
        preact = mm(normed2, up[i]) + up_bias_all[i]
        half = 0.5 * (1.0 + lax.erf(preact * (0.5**0.5)))
        bell = jnp.exp(-0.5 * preact * preact) * ((0.5 / jnp.pi) ** 0.5)
        hidden.append((preact * half).astype(BF))
        slope.append((half + preact * bell).astype(BF))

    grad_normed2 = 0.0
    terms_up, terms_down, sums_up = [], [], []
    for i in range(tp):
        grad_preact = (mm(grad_low, down_t[i]) * slope[i].astype(F32)).astype(BF)
        grad_normed2 = grad_normed2 + mm_nt(grad_preact, up[i])
        terms_up.append(mm_tn(normed2, grad_preact).astype(BF))
        terms_down.append(mm_tn(grad_low, hidden[i]).astype(BF))
        sums_up.append(jnp.sum(grad_preact.astype(F32), axis=0))
    grad_resid = grad_y + norm_back(grad_normed2, unit_two, scaled_two, norm2_gain)
    grad_resr = grad_resid.astype(BF)
    terms_out = [
        mm_tn(grad_resr, mixed[:, i * local_width : (i + 1) * local_width]).astype(BF)
        for i in range(tp)
    ]
    late = jnp.stack(
        [jnp.concatenate([terms_up[i], terms_down[i], terms_out[i]], axis=1) for i in range(tp)]
    ).reshape(tp * width, -1)
    late, grad_resr, hidden = lax.optimization_barrier((late, grad_resr, hidden))
    late = lax.psum_scatter(late, everyone, scatter_dimension=0, tiled=True)
    late = late.astype(F32)
    up_weight_grad = late[:, :local_hidden]
    down_weight_grad = late[:, local_hidden : 2 * local_hidden].T
    out_weight_grad = late[:, 2 * local_hidden :].T

    grad_project, head_sums = attend_back(
        grad_resr,
        gathered,
        edge_out,
        project,
        query_gain,
        query_bias,
        key_gain,
        ids,
        local_width,
    )
    output = resid + down_bias
    for i in range(tp):
        output = output + mm_nt(hidden[i], down_t[i])
    output = from_sequence(output.astype(BF), BF)

    grad_normed1 = 0.0
    terms_qkv, sums_qkv = [], []
    for i in range(tp):
        terms_qkv.append(mm_tn(normed1, grad_project[i]).astype(BF))
        sums_qkv.append(jnp.sum(grad_project[i].astype(F32), axis=0))
    early = jnp.stack(terms_qkv)
    early, grad_project = lax.optimization_barrier((early, grad_project))
    early = early.reshape(tp, -1, shard, edge_out)
    early = halve_over_fsdp(early, 1)
    early = add_halves(
        pick(early, me), lax.ppermute(pick(early, 1 - me), "tp", swap)
    )[None]
    step = 2
    while step < lax.axis_size("fsdp"):
        early = halve_over_fsdp(early, step)
        step *= 2
    early = early.reshape(shard, edge_out).astype(F32)
    for i in range(tp):
        grad_normed1 = grad_normed1 + mm_nt(grad_project[i], qkv[i])
    qkv_weight_grad = (
        early.reshape(shard, per, 3, lanes)
        .transpose(0, 2, 1, 3)
        .reshape(qkv_weight.shape)
    )
    input_grad = grad_resid + norm_back(grad_normed1, unit_one, scaled_one, norm1_gain)
    input_grad = from_sequence(input_grad, BF)

    vectors = [
        jnp.sum(grad_normed1 * unit_one, axis=0),
        jnp.sum(grad_normed1, axis=0),
        head_sums[0],
        head_sums[1],
        head_sums[2],
        jnp.sum(grad_resid, axis=0),
        jnp.sum(grad_normed2 * unit_two, axis=0),
        jnp.sum(grad_normed2, axis=0),
        jnp.sum(grad_y, axis=0),
        *sums_qkv,
        *sums_up,
    ]
    summed = sum_by_pairs(jnp.concatenate(vectors), everyone)
    pieces, start = [], 0
    for vector in vectors:
        pieces.append(summed[start : start + vector.shape[0]])
        start += vector.shape[0]
    gain_one, shift_one, gain_query, shift_query, gain_key = pieces[:5]
    sum_out, gain_two, shift_two, sum_down = pieces[5:9]
    qkv_bias_grad = jnp.where(me == 0, pieces[9], pieces[10])
    qkv_bias_grad = qkv_bias_grad.reshape(per, 3, lanes).transpose(1, 0, 2).reshape(qkv_bias.shape)
    up_bias_grad = jnp.where(me == 0, pieces[11], pieces[12])
    return (
        output,
        input_grad,
        gain_one,
        shift_one,
        qkv_weight_grad,
        qkv_bias_grad,
        gain_query,
        shift_query,
        gain_key,
        out_weight_grad,
        sum_out,
        gain_two,
        shift_two,
        up_weight_grad,
        up_bias_grad,
        down_weight_grad,
        sum_down,
    )


def solution(mesh):
    placed = (
        P(None, ("fsdp", "tp"), None),
        P(None, ("fsdp", "tp")),
        P(None, ("fsdp", "tp"), None),
        P(),
        P(),
        P("fsdp", None, "tp"),
        P(None, "tp"),
        P(),
        P(),
        P(),
        P("tp", "fsdp"),
        P(),
        P(),
        P(),
        P("fsdp", "tp"),
        P("tp"),
        P("tp", "fsdp"),
        P(),
    )
    return jax.shard_map(
        on_device,
        mesh=mesh,
        in_specs=placed,
        out_specs=(
            P(None, ("fsdp", "tp"), None),
            P(None, ("fsdp", "tp"), None),
            P(),
            P(),
            P("fsdp", None, "tp"),
            P(None, "tp"),
            P(),
            P(),
            P(),
            P("tp", "fsdp"),
            P(),
            P(),
            P(),
            P("fsdp", "tp"),
            P("tp"),
            P("tp", "fsdp"),
            P(),
        ),
        check_vma=False,
    )
```

```python
from functools import partial

import jax
import jax.numpy as jnp
from jax import lax
from jax.experimental import pallas as pl
from jax.experimental.pallas import tpu as pltpu
from jax.sharding import PartitionSpec as P

LEN = 1024
IMG_MOST = 256
BLOCK = 256
REACH = -(-(IMG_MOST - 1) // BLOCK)
EPSILON = 1e-06
BF = jnp.bfloat16
F32 = jnp.float32


def norm_parts(values):
    average = jnp.mean(values, axis=-1, keepdims=True)
    centred = values - average
    spread = jnp.mean(centred * centred, axis=-1, keepdims=True)
    scaled = lax.rsqrt(spread + EPSILON)
    return (centred * scaled, scaled)


def norm_back(grad_out, unit, scaled, gain):
    grad_unit = grad_out * gain
    first = jnp.mean(grad_unit, axis=-1, keepdims=True)
    second = jnp.mean(grad_unit * unit, axis=-1, keepdims=True)
    return scaled * (grad_unit - first - unit * second)


def mm(a, b):
    return jnp.dot(a, b, preferred_element_type=F32)


def mm_nt(a, b):
    return lax.dot_general(a, b, (((1,), (1,)), ((), ())), preferred_element_type=F32)


def mm_tn(a, b):
    return lax.dot_general(a, b, (((0,), (0,)), ((), ())), preferred_element_type=F32)


def key_range(block, count):
    return max(0, block - REACH), min(count, block + REACH + 1)


def head_means(values, table):
    high = values.astype(BF)
    low = (values - high.astype(F32)).astype(BF)
    return mm(high, table) + mm(low, table)


def head_norm_parts(values, table):
    centred = values - head_means(values, table)
    scaled = lax.rsqrt(head_means(centred * centred, table) + EPSILON)
    return (centred * scaled, scaled)


def attend_kernel(
    x_ref, w_ref, b_ref, table_ref, gain_ref, shift_ref, idc_ref, idr_ref, p_ref, mixed_ref,
    *, depth
):
    length = x_ref.shape[0]
    lanes = mixed_ref.shape[1]
    count = length // BLOCK
    project = mm(x_ref[...], w_ref[0]) + b_ref[0]
    p_ref[0] = project
    unit, _ = head_norm_parts(project[:, : 2 * lanes], table_ref[...])
    normed = (unit * gain_ref[...] + shift_ref[...]).astype(BF)
    queries = normed[:, :lanes] * jnp.asarray(depth ** (-0.5), BF)
    values = project[:, 2 * lanes :].astype(BF)
    heads = []
    for head in range(lanes // depth):
        columns = slice(head * depth, (head + 1) * depth)
        query = queries[:, columns]
        key = normed[:, lanes + head * depth : lanes + (head + 1) * depth]
        value = values[:, columns]
        value = jnp.concatenate([value, jnp.ones_like(value)], axis=1)
        rows = []
        for block in range(count):
            low, high = key_range(block, count)
            q = slice(block * BLOCK, (block + 1) * BLOCK)
            k = slice(low * BLOCK, high * BLOCK)
            scores = mm_nt(query[q], key[k])
            same = idc_ref[q, :] == idr_ref[:, k]
            weights = jnp.where(same, jnp.exp(scores), 0.0).astype(BF)
            both = mm(weights, value[k])
            rows.append(both[:, :depth] / both[:, depth : depth + 1])
        heads.append(jnp.concatenate(rows, axis=0))
    mixed_ref[...] = jnp.concatenate(heads, axis=1).astype(BF)


def attend_back_kernel(
    g_ref, w_ref, p_ref, table_ref, gain_ref, shift_ref, idc_ref, idr_ref, gp_ref, sums_ref,
    *, depth
):
    length = g_ref.shape[0]
    lanes = w_ref.shape[2]
    count = length // BLOCK
    scale = depth ** (-0.5)
    grad_mixed = mm(g_ref[...], w_ref[0]).astype(BF)
    unit, scaled = head_norm_parts(p_ref[0, :, : 2 * lanes], table_ref[...])
    normed = (unit * gain_ref[...] + shift_ref[...]).astype(BF)
    queries = normed[:, :lanes] * jnp.asarray(scale, BF)
    values = p_ref[0, :, 2 * lanes :].astype(BF)
    grad_queries, grad_keys, grad_values = [], [], []
    for head in range(lanes // depth):
        columns = slice(head * depth, (head + 1) * depth)
        query = queries[:, columns]
        key = normed[:, lanes + head * depth : lanes + (head + 1) * depth]
        value = values[:, columns]
        grad = grad_mixed[:, columns]
        grad_key = [None] * count
        grad_value = [None] * count
        grad_query = []
        for block in range(count):
            low, high = key_range(block, count)
            q = slice(block * BLOCK, (block + 1) * BLOCK)
            k = slice(low * BLOCK, high * BLOCK)
            scores = mm_nt(key[k], query[q])
            same = idc_ref[k, :] == idr_ref[:, q]
            raised = jnp.where(same, jnp.exp(scores), 0.0)
            weights = raised * (1.0 / jnp.sum(raised, axis=0, keepdims=True))
            grad_weights = mm_nt(value[k], grad[q])
            inner = jnp.sum(grad_weights * weights, axis=0, keepdims=True)
            grad_scores = (weights * (grad_weights - inner)).astype(BF)
            grad_query.append(mm_tn(grad_scores, key[k]) * scale)
            to_key = mm(grad_scores, query[q])
            to_value = mm(weights.astype(BF), grad[q])
            for i in range(low, high):
                piece = slice((i - low) * BLOCK, (i - low + 1) * BLOCK)
                grad_key[i] = to_key[piece] if grad_key[i] is None else grad_key[i] + to_key[piece]
                grad_value[i] = (
                    to_value[piece] if grad_value[i] is None else grad_value[i] + to_value[piece]
                )
        grad_queries.append(jnp.concatenate(grad_query, axis=0))
        grad_keys.append(jnp.concatenate(grad_key, axis=0))
        grad_values.append(jnp.concatenate(grad_value, axis=0))
    grads = jnp.concatenate(grad_queries + grad_keys, axis=1)
    grad_unit = grads * gain_ref[...]
    first = head_means(grad_unit, table_ref[...])
    second = head_means(grad_unit * unit, table_ref[...])
    gp_ref[0, :, : 2 * lanes] = (scaled * (grad_unit - first - unit * second)).astype(BF)
    gp_ref[0, :, 2 * lanes :] = jnp.concatenate(grad_values, axis=1).astype(BF)

    @pl.when(pl.program_id(0) == 0)
    def _():
        sums_ref[...] = jnp.zeros_like(sums_ref)

    sums_ref[0:1, :] += jnp.sum(grads * unit, axis=0, keepdims=True)
    sums_ref[1:2, :] += jnp.sum(grads, axis=0, keepdims=True)


def head_operands(query_gain, query_bias, key_gain):
    head = jnp.arange(4 * query_gain.shape[0]) // query_gain.shape[0]
    table = jnp.where(head[:, None] == head[None], 1.0 / query_gain.shape[0], 0.0).astype(BF)
    gain = jnp.concatenate([query_gain, query_gain, key_gain, key_gain])[None]
    none = jnp.zeros_like(query_bias)
    shift = jnp.concatenate([query_bias, query_bias, none, none])[None]
    return table, gain, shift


def add_halves(own, other):
    return (own.astype(F32) + other.astype(F32)).astype(BF)


def halve_over_fsdp(array, step):
    size = lax.axis_size("fsdp")
    assert size & (size - 1) == 0
    bit = lax.axis_index("fsdp") // step % 2
    pairs = array.reshape(array.shape[0], -1, 2, *array.shape[2:])
    own = lax.dynamic_index_in_dim(pairs, bit, 2, keepdims=False)
    other = lax.dynamic_index_in_dim(pairs, 1 - bit, 2, keepdims=False)
    return add_halves(own, lax.ppermute(other, "fsdp", [(i, i ^ step) for i in range(size)]))


def add_over_fsdp(vector, step):
    size = lax.axis_size("fsdp")
    return vector + lax.ppermute(vector, "fsdp", [(i, i ^ step) for i in range(size)])


def attend(normed, weight, bias, query_gain, query_bias, key_gain, ids, local_width):
    length, width = normed.shape
    tp = weight.shape[0]
    depth = query_gain.shape[0]
    lanes = 2 * depth
    per = local_width // lanes
    whole = lambda *shape: pl.BlockSpec(shape, lambda i: (0,) * len(shape))
    return pl.pallas_call(
        partial(attend_kernel, depth=depth),
        grid=(tp * per,),
        in_specs=[
            whole(length, width),
            pl.BlockSpec((1, width, 3 * lanes), lambda i: (i // per, 0, i % per)),
            pl.BlockSpec((1, 1, 3 * lanes), lambda i: (i // per, 0, i % per)),
            whole(2 * lanes, 2 * lanes),
            whole(1, 2 * lanes),
            whole(1, 2 * lanes),
            whole(length, 1),
            whole(1, length),
        ],
        out_specs=[
            pl.BlockSpec((1, length, 3 * lanes), lambda i: (i // per, 0, i % per)),
            pl.BlockSpec((length, lanes), lambda i: (0, i)),
        ],
        out_shape=[
            jax.ShapeDtypeStruct((tp, length, 3 * local_width), F32),
            jax.ShapeDtypeStruct((length, tp * local_width), BF),
        ],
        compiler_params=pltpu.CompilerParams(vmem_limit_bytes=56 * 2**20),
        cost_estimate=pl.CostEstimate(
            flops=2 * length * width * 3 * local_width * tp,
            bytes_accessed=length * local_width * tp * 16,
            transcendentals=length * 3 * BLOCK * tp * local_width // depth,
        ),
        name="attend",
    )(
        normed,
        weight,
        bias,
        *head_operands(query_gain, query_bias, key_gain),
        ids[:, None],
        ids[None],
    )


def attend_back(
    grad_rows, weight, out_column, project, query_gain, query_bias, key_gain, ids, local_width
):
    length, width = grad_rows.shape
    tp = weight.shape[0]
    depth = query_gain.shape[0]
    lanes = 2 * depth
    per = local_width // lanes
    first = out_column // lanes
    whole = lambda *shape: pl.BlockSpec(shape, lambda i: (0,) * len(shape))
    return pl.pallas_call(
        partial(attend_back_kernel, depth=depth),
        grid=(tp * per,),
        in_specs=[
            whole(length, width),
            pl.BlockSpec((1, width, lanes), lambda i: (i // per, 0, first + i % per)),
            pl.BlockSpec((1, length, 3 * lanes), lambda i: (i // per, 0, i % per)),
            whole(2 * lanes, 2 * lanes),
            whole(1, 2 * lanes),
            whole(1, 2 * lanes),
            whole(length, 1),
            whole(1, length),
        ],
        out_specs=[
            pl.BlockSpec((1, length, 3 * lanes), lambda i: (i // per, 0, i % per)),
            whole(2, 2 * lanes),
        ],
        out_shape=[
            jax.ShapeDtypeStruct((tp, length, 3 * local_width), BF),
            jax.ShapeDtypeStruct((2, 2 * lanes), F32),
        ],
        compiler_params=pltpu.CompilerParams(vmem_limit_bytes=56 * 2**20),
        cost_estimate=pl.CostEstimate(
            flops=8 * length * width * local_width * tp,
            bytes_accessed=length * local_width * tp * 18,
            transcendentals=length * 3 * BLOCK * tp * local_width // depth,
        ),
        name="attend_back",
    )(
        grad_rows,
        weight,
        project,
        *head_operands(query_gain, query_bias, key_gain),
        ids[:, None],
        ids[None],
    )


def on_device(
    inputs,
    image_ids,
    cotangent,
    norm1_gain,
    norm1_bias,
    qkv_weight,
    qkv_bias,
    query_gain,
    query_bias,
    key_gain,
    out_weight,
    out_bias,
    norm2_gain,
    norm2_bias,
    up_weight,
    up_bias,
    down_weight,
    down_bias,
):
    batches, rows_here, width = inputs.shape
    tp = lax.axis_size("tp")
    me = lax.axis_index("tp")
    assert batches == 2 and tp == 2 and rows_here * tp == LEN
    everyone = ("tp", "fsdp")
    shard = qkv_weight.shape[0]
    local_width = qkv_weight.shape[2]
    local_hidden = up_weight.shape[1]
    depth = query_gain.shape[0]
    lanes = 2 * depth
    per = local_width // lanes
    swap = [(0, 1), (1, 0)]

    def pick(array, index):
        return lax.dynamic_index_in_dim(array, index, 0, keepdims=False)

    def in_order(own, other):
        return jnp.where(
            me == 0, jnp.concatenate([own, other], 0), jnp.concatenate([other, own], 0)
        )

    def to_sequence(array):
        return in_order(pick(array, me), lax.ppermute(pick(array, 1 - me), "tp", swap))

    def from_sequence(array, dtype):
        halves = array.reshape(2, rows_here, width)
        other = lax.ppermute(pick(halves, 1 - me).astype(dtype), "tp", swap).astype(array.dtype)
        own = pick(halves, me)
        return jnp.where(me == 0, jnp.stack([own, other]), jnp.stack([other, own]))

    packed = jnp.concatenate(
        [
            qkv_weight.reshape(shard, 3, per, lanes).transpose(0, 2, 1, 3).reshape(shard, -1),
            out_weight.T,
            up_weight,
            down_weight.T,
        ],
        axis=1,
    )
    gathered = lax.all_gather(packed, everyone, axis=0, tiled=True).reshape(tp, width, -1)
    edge_out = 3 * local_width
    edge_up = edge_out + local_width
    edge_down = edge_up + local_hidden
    out_t = [gathered[i, :, edge_out:edge_up] for i in range(tp)]
    up = [gathered[i, :, edge_up:edge_down] for i in range(tp)]
    down_t = [gathered[i, :, edge_down:] for i in range(tp)]
    qkv = [gathered[i, :, :edge_out] for i in range(tp)]

    biases = jnp.concatenate(
        [qkv_bias.reshape(3, per, lanes).transpose(1, 0, 2).reshape(-1), up_bias]
    )
    biases = in_order(biases[None], lax.ppermute(biases, "tp", swap)[None])
    qkv_bias_all = biases[:, None, :edge_out]
    up_bias_all = biases[:, edge_out:]

    tokens_in = to_sequence(inputs).astype(F32)
    ids = to_sequence(image_ids)
    grad_low = to_sequence(cotangent)
    grad_y = grad_low.astype(F32)

    unit_one, scaled_one = norm_parts(tokens_in)
    normed1 = (unit_one * norm1_gain + norm1_bias).astype(BF)
    project, mixed = attend(
        normed1, gathered, qkv_bias_all, query_gain, query_bias, key_gain, ids, local_width
    )
    resid = tokens_in + out_bias
    for i in range(tp):
        resid = resid + mm_nt(mixed[:, i * local_width : (i + 1) * local_width], out_t[i])
    unit_two, scaled_two = norm_parts(resid)
    normed2 = (unit_two * norm2_gain + norm2_bias).astype(BF)

    hidden, slope = [], []
    for i in range(tp):
        preact = mm(normed2, up[i]) + up_bias_all[i]
        half = 0.5 * (1.0 + lax.erf(preact * (0.5**0.5)))
        bell = jnp.exp(-0.5 * preact * preact) * ((0.5 / jnp.pi) ** 0.5)
        hidden.append((preact * half).astype(BF))
        slope.append((half + preact * bell).astype(BF))

    grad_normed2 = 0.0
    terms_up, terms_down, sums_up = [], [], []
    for i in range(tp):
        grad_preact = (mm(grad_low, down_t[i]) * slope[i].astype(F32)).astype(BF)
        grad_normed2 = grad_normed2 + mm_nt(grad_preact, up[i])
        terms_up.append(mm_tn(normed2, grad_preact).astype(BF))
        terms_down.append(mm_tn(grad_low, hidden[i]).astype(BF))
        sums_up.append(jnp.sum(grad_preact.astype(F32), axis=0))
    grad_resid = grad_y + norm_back(grad_normed2, unit_two, scaled_two, norm2_gain)
    grad_resr = grad_resid.astype(BF)
    terms_out = [
        mm_tn(grad_resr, mixed[:, i * local_width : (i + 1) * local_width]).astype(BF)
        for i in range(tp)
    ]
    late = jnp.stack(
        [jnp.concatenate([terms_up[i], terms_down[i], terms_out[i]], axis=1) for i in range(tp)]
    ).reshape(tp * width, -1)
    late, grad_resr, hidden = lax.optimization_barrier((late, grad_resr, hidden))
    late = lax.psum_scatter(late, everyone, scatter_dimension=0, tiled=True)
    late = late.astype(F32)
    up_weight_grad = late[:, :local_hidden]
    down_weight_grad = late[:, local_hidden : 2 * local_hidden].T
    out_weight_grad = late[:, 2 * local_hidden :].T

    grad_project, head_sums = attend_back(
        grad_resr,
        gathered,
        edge_out,
        project,
        query_gain,
        query_bias,
        key_gain,
        ids,
        local_width,
    )
    output = resid + down_bias
    for i in range(tp):
        output = output + mm_nt(hidden[i], down_t[i])
    output = from_sequence(output.astype(BF), BF)

    grad_normed1 = 0.0
    terms_qkv, sums_qkv = [], []
    for i in range(tp):
        terms_qkv.append(mm_tn(normed1, grad_project[i]).astype(BF))
        sums_qkv.append(jnp.sum(grad_project[i].astype(F32), axis=0))
    early = jnp.stack(terms_qkv)
    early, grad_project = lax.optimization_barrier((early, grad_project))
    early = halve_over_fsdp(early.reshape(tp, -1, shard, edge_out), 1)
    for i in range(tp):
        grad_normed1 = grad_normed1 + mm_nt(grad_project[i], qkv[i])
    input_grad = grad_resid + norm_back(grad_normed1, unit_one, scaled_one, norm1_gain)
    input_grad = from_sequence(input_grad, BF)

    vectors = [
        jnp.sum(grad_normed1 * unit_one, axis=0),
        jnp.sum(grad_normed1, axis=0),
        head_sums[0, :depth] + head_sums[0, depth : 2 * depth],
        head_sums[1, :depth] + head_sums[1, depth : 2 * depth],
        head_sums[0, 2 * depth : 3 * depth] + head_sums[0, 3 * depth :],
        jnp.sum(grad_resid, axis=0),
        jnp.sum(grad_normed2 * unit_two, axis=0),
        jnp.sum(grad_normed2, axis=0),
        jnp.sum(grad_y, axis=0),
        *sums_qkv,
        *sums_up,
    ]
    summed, early = lax.optimization_barrier((jnp.concatenate(vectors), early))
    received = lax.ppermute(pick(early, 1 - me), "tp", swap)
    summed = summed + lax.ppermute(summed, "tp", swap)
    early = add_halves(pick(early, me), received)[None]
    step = 1
    while step < lax.axis_size("fsdp"):
        summed, early = lax.optimization_barrier((summed, early))
        if 2 * step < lax.axis_size("fsdp"):
            early = halve_over_fsdp(early, 2 * step)
        summed = add_over_fsdp(summed, step)
        step *= 2
    early = early.reshape(shard, edge_out).astype(F32)
    qkv_weight_grad = (
        early.reshape(shard, per, 3, lanes)
        .transpose(0, 2, 1, 3)
        .reshape(qkv_weight.shape)
    )
    pieces, start = [], 0
    for vector in vectors:
        pieces.append(summed[start : start + vector.shape[0]])
        start += vector.shape[0]
    gain_one, shift_one, gain_query, shift_query, gain_key = pieces[:5]
    sum_out, gain_two, shift_two, sum_down = pieces[5:9]
    qkv_bias_grad = jnp.where(me == 0, pieces[9], pieces[10])
    qkv_bias_grad = qkv_bias_grad.reshape(per, 3, lanes).transpose(1, 0, 2).reshape(qkv_bias.shape)
    up_bias_grad = jnp.where(me == 0, pieces[11], pieces[12])
    return (
        output,
        input_grad,
        gain_one,
        shift_one,
        qkv_weight_grad,
        qkv_bias_grad,
        gain_query,
        shift_query,
        gain_key,
        out_weight_grad,
        sum_out,
        gain_two,
        shift_two,
        up_weight_grad,
        up_bias_grad,
        down_weight_grad,
        sum_down,
    )


def solution(mesh):
    placed = (
        P(None, ("fsdp", "tp"), None),
        P(None, ("fsdp", "tp")),
        P(None, ("fsdp", "tp"), None),
        P(),
        P(),
        P("fsdp", None, "tp"),
        P(None, "tp"),
        P(),
        P(),
        P(),
        P("tp", "fsdp"),
        P(),
        P(),
        P(),
        P("fsdp", "tp"),
        P("tp"),
        P("tp", "fsdp"),
        P(),
    )
    return jax.shard_map(
        on_device,
        mesh=mesh,
        in_specs=placed,
        out_specs=(
            P(None, ("fsdp", "tp"), None),
            P(None, ("fsdp", "tp"), None),
            P(),
            P(),
            P("fsdp", None, "tp"),
            P(None, "tp"),
            P(),
            P(),
            P(),
            P("tp", "fsdp"),
            P(),
            P(),
            P(),
            P("fsdp", "tp"),
            P("tp"),
            P("tp", "fsdp"),
            P(),
        ),
        check_vma=False,
    )
```
